32 devices in a mesh: dp: 32 (over z, y, x, core).
Axes of the slice: x: 2, y: 2, z: 4, core: 2. Of those that a mesh axis runs over, the one named last changes fastest.
Arguments:
- act_in: bfloat16 [2048, 7, 7, 512], P('dp')
- shortcut: bfloat16 [2048, 7, 7, 2048], P('dp')
- labels: int32 [2048], P('dp')
- w_conv: float32 [512, 2048], replicated
- bn_gamma: float32 [2048], replicated
- bn_beta: float32 [2048], replicated
- w_fc: float32 [2048, 8142], replicated
- fc_bias: float32 [8142], replicated
- vel_conv: float32 [512, 2048], replicated
- vel_gamma: float32 [2048], replicated
- vel_beta: float32 [2048], replicated
- vel_fc: float32 [2048, 8142], replicated
- vel_bias: float32 [8142], replicated
- learn_rate: float32 [], replicated
Outputs:
- output 1: float32 [512, 2048], replicated
- output 2: float32 [2048], replicated
- output 3: float32 [2048], replicated
- output 4: float32 [2048, 8142], replicated
- output 5: float32 [8142], replicated
- output 6: float32 [512, 2048], replicated
- output 7: float32 [2048], replicated
- output 8: float32 [2048], replicated
- output 9: float32 [2048, 8142], replicated
- output 10: float32 [8142], replicated
- output 11: float32 [], replicated
All inputs are finite; a program needn't handle non-finite values.
Results may differ from the reference program's by a relative error of at most 0.00886188.
Values sent between devices are 32-bit elements.
A program may use at most 1.25 GiB of HBM per device.

```python
import jax
import jax.numpy as jnp
from jax import lax

B_DEV = 64
DP = 32
SIDE = 7
C_MID = 512
C_OUT = 2048
CLASSES = 8142

BN_EPS = 1e-5
SMOOTHING = 0.1
MOMENTUM = 0.9
TRUST_COEF = 0.001
WEIGHT_DECAY = 5e-5


def setup_inputs(seed: int = 0) -> dict:
    root_key = jax.random.key(seed)
    sub_keys = jax.random.split(root_key, 16)
    global_rows = DP * B_DEV
    step_scale = 2.5
    dev_shift = 0.5 * jax.random.normal(sub_keys[0], (DP, 1, 1, 1, C_MID), jnp.float32)
    act_in = jax.nn.relu(jax.random.normal(sub_keys[1], (DP, B_DEV, SIDE, SIDE, C_MID), jnp.float32) + dev_shift)
    act_in = act_in.reshape(global_rows, SIDE, SIDE, C_MID).astype(jnp.bfloat16)
    shortcut = jax.nn.relu(jax.random.normal(sub_keys[2], (global_rows, SIDE, SIDE, C_OUT), jnp.float32)).astype(jnp.bfloat16)
    labels = jax.random.randint(sub_keys[3], (global_rows,), 0, CLASSES, jnp.int32)
    w_conv = C_MID ** -0.5 * jax.random.normal(sub_keys[4], (C_MID, C_OUT), jnp.float32)
    bn_gamma = jax.random.uniform(sub_keys[5], (C_OUT,), jnp.float32, 0.5, 1.5)
    bn_beta = 0.5 * jax.random.normal(sub_keys[6], (C_OUT,), jnp.float32)
    w_fc = C_OUT ** -0.5 * jax.random.normal(sub_keys[7], (C_OUT, CLASSES), jnp.float32)
    fc_bias = 0.5 * jax.random.normal(sub_keys[8], (CLASSES,), jnp.float32)
    vel_conv = 0.001 * step_scale * C_MID ** -0.5 * jax.random.normal(sub_keys[9], (C_MID, C_OUT), jnp.float32)
    vel_gamma = 0.5 * step_scale * (global_rows * C_OUT) ** -0.5 * jax.random.normal(sub_keys[10], (C_OUT,), jnp.float32)
    vel_beta = 0.5 * step_scale * (global_rows * C_OUT) ** -0.5 * jax.random.normal(sub_keys[11], (C_OUT,), jnp.float32)
    vel_fc = 0.001 * step_scale * C_OUT ** -0.5 * jax.random.normal(sub_keys[12], (C_OUT, CLASSES), jnp.float32)
    vel_bias = 0.9 * step_scale * (global_rows * CLASSES) ** -0.5 * jax.random.normal(sub_keys[13], (CLASSES,), jnp.float32)
    learn_rate = jax.random.uniform(sub_keys[14], (), jnp.float32, 1.0, 4.0)
    return {'act_in': act_in, 'shortcut': shortcut, 'labels': labels, 'w_conv': w_conv, 'bn_gamma': bn_gamma, 'bn_beta': bn_beta, 'w_fc': w_fc, 'fc_bias': fc_bias, 'vel_conv': vel_conv, 'vel_gamma': vel_gamma, 'vel_beta': vel_beta, 'vel_fc': vel_fc, 'vel_bias': vel_bias, 'learn_rate': learn_rate}


def group_loss(params, act_grp, short_grp, label_grp):
    w_conv, bn_gamma, bn_beta, w_fc, fc_bias = params
    pos_count = B_DEV * SIDE * SIDE
    conv_out = jnp.dot(act_grp.reshape(pos_count, C_MID), w_conv.astype(jnp.bfloat16), preferred_element_type=jnp.float32)
    batch_mean = jnp.mean(conv_out, axis=0)
    centered = conv_out - batch_mean
    batch_var = jnp.mean(jnp.square(centered), axis=0)
    x_hat = centered * lax.rsqrt(batch_var + BN_EPS)
    activ = jax.nn.relu(x_hat * bn_gamma + bn_beta + short_grp.reshape(pos_count, C_OUT).astype(jnp.float32))
    pooled = jnp.mean(activ.reshape(B_DEV, SIDE * SIDE, C_OUT), axis=1)
    logits = jnp.dot(pooled.astype(jnp.bfloat16), w_fc.astype(jnp.bfloat16), preferred_element_type=jnp.float32) + fc_bias
    log_prob = jax.nn.log_softmax(logits, axis=-1)
    one_hot_lab = (label_grp[:, None] == jnp.arange(CLASSES)[None, :]).astype(jnp.float32)
    target = SMOOTHING / CLASSES + (1.0 - SMOOTHING) * one_hot_lab
    return -jnp.sum(target * log_prob)


def lars_update(weight, gradient, velocity, learn_rate):
    w_norm = jnp.sqrt(jnp.sum(jnp.square(weight)))
    g_norm = jnp.sqrt(jnp.sum(jnp.square(gradient)))
    trust = TRUST_COEF * w_norm / (g_norm + WEIGHT_DECAY * w_norm)
    new_vel = MOMENTUM * velocity + learn_rate * trust * (gradient + WEIGHT_DECAY * weight)
    return weight - new_vel, new_vel


def reference(act_in, shortcut, labels, w_conv, bn_gamma, bn_beta, w_fc, fc_bias, vel_conv, vel_gamma, vel_beta, vel_fc, vel_bias, learn_rate):
    params = (w_conv, bn_gamma, bn_beta, w_fc, fc_bias)
    grad_fn = jax.value_and_grad(group_loss)
    global_rows = DP * B_DEV

    def scan_body(carry, group_batch):
        loss_sum, grad_sum = carry
        loss_val, grads = grad_fn(params, group_batch[0], group_batch[1], group_batch[2])
        return (loss_sum + loss_val, jax.tree.map(jnp.add, grad_sum, grads)), None

    init_carry = (jnp.zeros((), jnp.float32), jax.tree.map(jnp.zeros_like, params))
    group_data = (act_in.reshape(DP, B_DEV, SIDE, SIDE, C_MID), shortcut.reshape(DP, B_DEV, SIDE, SIDE, C_OUT), labels.reshape(DP, B_DEV))
    (loss_sum, grad_sum), unused_out = lax.scan(scan_body, init_carry, group_data)
    g_conv, g_gamma, g_beta, g_fc, g_bias = [grad_part / global_rows for grad_part in grad_sum]
    conv_new, conv_vel_new = lars_update(w_conv, g_conv, vel_conv, learn_rate)
    fc_new, fc_vel_new = lars_update(w_fc, g_fc, vel_fc, learn_rate)
    gamma_vel_new = MOMENTUM * vel_gamma + learn_rate * g_gamma
    beta_vel_new = MOMENTUM * vel_beta + learn_rate * g_beta
    bias_vel_new = MOMENTUM * vel_bias + learn_rate * g_bias
    return (conv_new, bn_gamma - gamma_vel_new, bn_beta - beta_vel_new, fc_new, fc_bias - bias_vel_new, conv_vel_new, gamma_vel_new, beta_vel_new, fc_vel_new, bias_vel_new, loss_sum / global_rows)
```

```python
import functools

import jax
import jax.numpy as jnp
from jax import lax
from jax.experimental import pallas as pl
from jax.experimental.pallas import tpu as pltpu
from jax.sharding import PartitionSpec as P


BN_EPS = 1e-5
SMOOTHING = 0.1
MOMENTUM = 0.9
TRUST_COEF = 0.001
WEIGHT_DECAY = 5e-5
TILE = 256


def prep_kernel(p_ref, pb_ref, pt_ref):
    block = p_ref[...]
    pb_ref[...] = block.astype(jnp.bfloat16)
    pt_ref[...] = block.T.astype(jnp.bfloat16)


def prep(p_all):
    rows, chans = p_all.shape
    step = 256
    return pl.pallas_call(
        prep_kernel,
        grid=(rows // step,),
        in_specs=[pl.BlockSpec((step, chans), lambda i: (i, 0))],
        out_specs=[pl.BlockSpec((step, chans), lambda i: (i, 0)), pl.BlockSpec((chans, step), lambda i: (0, i))],
        out_shape=[jax.ShapeDtypeStruct((rows, chans), jnp.bfloat16), jax.ShapeDtypeStruct((chans, rows), jnp.bfloat16)],
        cost_estimate=pl.CostEstimate(flops=10**9, bytes_accessed=8 * rows * chans, transcendentals=0),
        name='prep',
    )(p_all)


def tile_grad(w, pb_ref, pt_ref, stat_ref, lab_ref, bias_row, tile_idx, classes):
    rows = w.shape[0]
    images = pb_ref.shape[0]
    bias_col = jnp.broadcast_to(bias_row, (128, rows)).T[:, :1]
    logit = jnp.dot(w.astype(jnp.bfloat16), pt_ref[...], preferred_element_type=jnp.float32) + bias_col
    prob = jnp.exp((logit - stat_ref[0:1, :]) - stat_ref[1:2, :])
    cls = tile_idx * rows + lax.broadcasted_iota(jnp.int32, (rows, images), 0)
    target = jnp.where(cls == lab_ref[0:1, :], SMOOTHING / classes + (1.0 - SMOOTHING), SMOOTHING / classes)
    dlog = (prob - target) * (1.0 / images)
    d_bias = jnp.sum(dlog, axis=1, keepdims=True)
    grad = jnp.dot(dlog.astype(jnp.bfloat16), pb_ref[...], preferred_element_type=jnp.float32)
    return grad, d_bias


def norm_kernel(classes, idx_ref, w_ref, pb_ref, pt_ref, stat_ref, lab_ref, bias_ref, out_ref):
    tile = idx_ref[0]
    w = w_ref[...]
    grad, _ = tile_grad(w, pb_ref, pt_ref, stat_ref, lab_ref, bias_ref[0], tile, classes)
    row = tile * TILE + lax.broadcasted_iota(jnp.int32, w.shape, 0)
    keep = row < classes
    out_ref[0:1, :] = jnp.sum(jnp.where(keep, w * w, 0.0), axis=0, keepdims=True)
    out_ref[1:2, :] = jnp.sum(jnp.where(keep, grad * grad, 0.0), axis=0, keepdims=True)


def update_kernel(classes, coef_ref, w_ref, v_ref, pb_ref, pt_ref, stat_ref, lab_ref, bias_ref, vbias_ref, wn_ref, vn_ref, bn_ref, vbn_ref):
    tile = pl.program_id(0)
    w = w_ref[...]
    bias_row = bias_ref[0]
    grad, d_bias = tile_grad(w, pb_ref, pt_ref, stat_ref, lab_ref, bias_row, tile, classes)
    v_new = MOMENTUM * v_ref[...] + coef_ref[0] * (grad + WEIGHT_DECAY * w)
    vn_ref[...] = v_new
    wn_ref[...] = w - v_new
    d_row = jnp.broadcast_to(d_bias, (d_bias.shape[0], 128)).T[0:1, :]
    vb_new = MOMENTUM * vbias_ref[0] + coef_ref[1] * d_row
    vbn_ref[0] = vb_new
    bn_ref[0] = bias_row - vb_new


def resident(shape):
    return pl.BlockSpec(shape, lambda *_: (0,) * len(shape), pipeline_mode=pl.Buffered(1))


def head_norms(tile_idx, w_t, pb, pt, stat, lab, bias_tiles):
    classes, chans = w_t.shape
    images = pb.shape[0]
    grid_spec = pltpu.PrefetchScalarGridSpec(
        num_scalar_prefetch=1,
        grid=(1,),
        in_specs=[
            pl.BlockSpec((TILE, chans), lambda i, idx: (idx[0], 0), pipeline_mode=pl.Buffered(1)),
            resident((images, chans)),
            resident((chans, images)),
            resident((2, images)),
            resident((1, images)),
            pl.BlockSpec((1, 1, TILE), lambda i, idx: (idx[0], 0, 0)),
        ],
        out_specs=pl.BlockSpec((2, chans), lambda i, idx: (0, 0)),
    )
    return pl.pallas_call(
        functools.partial(norm_kernel, classes),
        grid_spec=grid_spec,
        out_shape=jax.ShapeDtypeStruct((2, chans), jnp.float32),
        compiler_params=pltpu.CompilerParams(vmem_limit_bytes=56 * 2**20),
        cost_estimate=pl.CostEstimate(flops=4 * TILE * chans * images, bytes_accessed=20 * 2**20, transcendentals=TILE * images),
        name='head_norms',
    )(tile_idx, w_t, pb, pt, stat, lab, bias_tiles)


def head_update(coef, w_t, v_t, pb, pt, stat, lab, bias_tiles, vbias_tiles):
    classes, chans = w_t.shape
    images = pb.shape[0]
    tiles = pl.cdiv(classes, TILE)
    row_block = pl.BlockSpec((TILE, chans), lambda i: (i, 0))
    vec_block = pl.BlockSpec((1, 1, TILE), lambda i: (i, 0, 0))
    return pl.pallas_call(
        functools.partial(update_kernel, classes),
        grid=(tiles,),
        in_specs=[
            pl.BlockSpec(memory_space=pltpu.SMEM),
            row_block,
            row_block,
            resident((images, chans)),
            resident((chans, images)),
            resident((2, images)),
            resident((1, images)),
            vec_block,
            vec_block,
        ],
        out_specs=[row_block, row_block, vec_block, vec_block],
        out_shape=[
            jax.ShapeDtypeStruct(w_t.shape, jnp.float32),
            jax.ShapeDtypeStruct(w_t.shape, jnp.float32),
            jax.ShapeDtypeStruct(bias_tiles.shape, jnp.float32),
            jax.ShapeDtypeStruct(bias_tiles.shape, jnp.float32),
        ],
        compiler_params=pltpu.CompilerParams(vmem_limit_bytes=60 * 2**20),
        cost_estimate=pl.CostEstimate(flops=4 * classes * chans * images, bytes_accessed=16 * classes * chans, transcendentals=classes * images),
        name='head_update',
    )(coef, w_t, v_t, pb, pt, stat, lab, bias_tiles, vbias_tiles)


def solution(mesh):
    groups = mesh.shape['dp']

    def local_step(act_in, shortcut, labels, w_conv, bn_gamma, bn_beta, w_fc, fc_bias, vel_conv, vel_gamma, vel_beta, vel_fc, vel_bias, learn_rate):
        per_dev = act_in.shape[0]
        global_rows = per_dev * groups
        spatial = act_in.shape[1] * act_in.shape[2]
        c_mid = act_in.shape[3]
        c_out = shortcut.shape[3]
        classes = w_fc.shape[1]
        pos_count = per_dev * spatial
        tiles = pl.cdiv(classes, TILE)
        act_grid = act_in.reshape(per_dev, spatial, c_mid)
        conv_out = jnp.einsum('bpc,cd->bpd', act_grid, w_conv.astype(jnp.bfloat16), preferred_element_type=jnp.float32)
        batch_mean = jnp.mean(conv_out, axis=(0, 1))
        centered = conv_out - batch_mean
        inv_std = lax.rsqrt(jnp.mean(jnp.square(centered), axis=(0, 1)) + BN_EPS)
        x_hat = centered * inv_std
        pre_act = x_hat * bn_gamma + bn_beta + shortcut.reshape(per_dev, spatial, c_out).astype(jnp.float32)
        pooled = jnp.mean(jax.nn.relu(pre_act), axis=1)

        p_all = lax.all_gather(pooled, 'dp', axis=0, tiled=True)

        pooled_bf = pooled.astype(jnp.bfloat16)
        fc_bf = w_fc.astype(jnp.bfloat16)
        logits = jnp.dot(pooled_bf, fc_bf, preferred_element_type=jnp.float32)
        logits = logits + fc_bias
        row_max = jnp.max(logits, axis=-1)
        row_log = jnp.log(jnp.sum(jnp.exp(logits - row_max[:, None]), axis=-1))
        stat_own = jnp.stack([row_max, row_log, labels.astype(jnp.float32)])
        stat_all = lax.all_gather(stat_own, 'dp', axis=1, tiled=True)
        stat = stat_all[0:2]
        lab = stat_all[2:3].astype(jnp.int32)

        log_prob = (logits - row_max[:, None]) - row_log[:, None]
        one_hot_lab = (labels[:, None] == jnp.arange(classes, dtype=jnp.int32)[None, :]).astype(jnp.float32)
        target = SMOOTHING / classes + (1.0 - SMOOTHING) * one_hot_lab
        loss_part = -jnp.sum(target * log_prob) / global_rows
        d_logits_bf = ((jnp.exp(log_prob) - target) / global_rows).astype(jnp.bfloat16)
        d_pool = jnp.einsum('bk,ck->bc', d_logits_bf, fc_bf, preferred_element_type=jnp.float32) / spatial
        d_pre = jnp.where(pre_act > 0, d_pool[:, None, :], 0.0)
        d_beta = jnp.sum(d_pre, axis=(0, 1))
        d_gamma = jnp.sum(d_pre * x_hat, axis=(0, 1))
        d_conv_out = (bn_gamma * inv_std) * (d_pre - d_beta / pos_count - x_hat * (d_gamma / pos_count))
        d_conv = jnp.einsum('bpc,bpd->cd', act_grid, d_conv_out.astype(jnp.bfloat16), preferred_element_type=jnp.float32)

        loss_row = jnp.full((1, c_out), loss_part)
        packed = jnp.concatenate([d_conv, d_gamma[None], d_beta[None], loss_row, jnp.zeros((5, c_out), jnp.float32)], axis=0)
        packed = lax.psum(packed, 'dp')
        g_conv = packed[:c_mid]
        g_gamma, g_beta, loss_val = packed[c_mid], packed[c_mid + 1], packed[c_mid + 2, 0]

        pb, pt = prep(p_all)
        w_t, v_t = w_fc.T, vel_fc.T
        pad = tiles * TILE - classes
        bias_tiles = jnp.pad(fc_bias, (0, pad)).reshape(tiles, 1, TILE)
        vbias_tiles = jnp.pad(vel_bias, (0, pad)).reshape(tiles, 1, TILE)
        idx = lax.axis_index('dp').astype(jnp.int32).reshape(1)
        norms = lax.psum(jnp.sum(head_norms(idx, w_t, pb, pt, stat, lab, bias_tiles), axis=1), 'dp')
        w_norm, g_norm = jnp.sqrt(norms[0]), jnp.sqrt(norms[1])
        trust = TRUST_COEF * w_norm / (g_norm + WEIGHT_DECAY * w_norm)
        coef = jnp.stack([learn_rate * trust, learn_rate])
        wn_t, vn_t, bn_t, vbn_t = head_update(coef, w_t, v_t, pb, pt, stat, lab, bias_tiles, vbias_tiles)

        wc_norm = jnp.sqrt(jnp.sum(jnp.square(w_conv)))
        gc_norm = jnp.sqrt(jnp.sum(jnp.square(g_conv)))
        trust_c = TRUST_COEF * wc_norm / (gc_norm + WEIGHT_DECAY * wc_norm)
        conv_vel_new = MOMENTUM * vel_conv + learn_rate * trust_c * (g_conv + WEIGHT_DECAY * w_conv)
        gamma_vel_new = MOMENTUM * vel_gamma + learn_rate * g_gamma
        beta_vel_new = MOMENTUM * vel_beta + learn_rate * g_beta
        bias_new = bn_t.reshape(-1)[:classes]
        vbias_new = vbn_t.reshape(-1)[:classes]
        return (w_conv - conv_vel_new, bn_gamma - gamma_vel_new, bn_beta - beta_vel_new, wn_t.T, bias_new, conv_vel_new, gamma_vel_new, beta_vel_new, vn_t.T, vbias_new, loss_val)

    return jax.shard_map(local_step, mesh=mesh, in_specs=(P('dp'),) * 3 + (P(),) * 11, out_specs=(P(),) * 11, check_vma=False)
```
